32 devices in a mesh: gx: 4 (over y, x), gy: 8 (over z, core).
Axes of the slice: x: 2, y: 2, z: 4, core: 2. Of those that a mesh axis runs over, the one named last changes fastest.
Arguments:
- traces: bfloat16 [8, 16, 128, 256], P('gx', 'gy'), may hold values from -6 to 6
- aperture: int32 [8, 16, 9], P('gx', 'gy'), may hold values 0 or 1
- geometry: int32 [8, 16, 3, 128], P('gx', 'gy'), may hold values from 0 to 63, as said below
- trace_weight: bfloat16 [8, 16, 128], P('gx', 'gy'), may hold values from 0.0087890625 to 0.03515625
- class_weight: float32 [14], replicated, may hold values from 0.3 to 1.5
- traveltime: int32 [14, 256], replicated, may hold values from 0 to 1114
Outputs:
- image: float32 [64, 64, 256], P('gx', 'gy')
The draws below stay inside these ranges and needn't reach their ends.
Inputs may be any that keep to these rules, and one draw needn't show every extreme that they name: Row 0 of a trace's geometry is an inline midpoint among the 16 image columns of its block's tile, row 1 a crossline midpoint among its tile's 8 columns, row 2 an offset class below 8.
All inputs are finite; a program needn't handle non-finite values. No bound on the sum of `aperture` on one device may be relied on, other than what follows from the above.
Results may differ from the reference program's by a relative error of at most 0.0029.
Values may be sent and summed in bfloat16 or wider, within the bound.
A program may use at most 64 MiB of HBM per device.

```python
import math
import jax
import jax.numpy as jnp
from jax import lax

NS = 256
NTIME = 256
TR = 128
NH = 8
BB = 2
PX = 16
PY = 8
DSTEP = 8
NC = 14
NBX = 8
NBY = 16
NX = 64
NY = 64
N_GX = 4
N_GY = 8


def draw_geometry(key, part):
    keys = jax.random.split(jax.random.fold_in(key, 11), 3)
    block_x = jnp.arange(NBX, dtype=jnp.int32)[:, None, None] // BB
    block_y = jnp.arange(NBY, dtype=jnp.int32)[None, :, None] // BB
    inline = block_x * PX + jax.random.randint(keys[0], (NBX, NBY, TR), 0, PX)
    crossline = block_y * PY + jax.random.randint(keys[1], (NBX, NBY, TR), 0, PY)
    offset_class = jax.random.randint(keys[2], (NBX, NBY, TR), 0, NH)
    return jnp.stack([inline, crossline, offset_class], axis=2).astype(jnp.int32)


def draw_traveltime(key, part):
    level = jnp.arange(NC, dtype=jnp.int32)[:, None]
    sample = jnp.arange(NTIME, dtype=jnp.int32)[None, :]
    raw = jax.random.randint(jax.random.fold_in(key, 23), (NC, NTIME), 0, 1 << 20)
    extra = raw % (4 * level + 4)
    return (4 * sample + 3 * level + extra).astype(jnp.int32)


def touch_ends(entries, key, low, high):
    extent = entries.shape
    index_at = [jax.random.randint(jax.random.fold_in(key, axis), (), 0, extent[axis]) for axis in range(len(extent))]
    entries = entries.at[tuple(index_at)].set(low)
    longest = extent.index(max(extent))
    index_at[longest] = (index_at[longest] + 1) % extent[longest]
    return entries.at[tuple(index_at)].set(high)


def levels(stream_key, dims, pieces, least, largest):
    gain = 1.0
    for axis_at, blocks in pieces:
        steps = jax.random.uniform(jax.random.fold_in(jax.random.fold_in(stream_key, 6), axis_at), (blocks,), jnp.float32, least / len(pieces), largest / len(pieces))
        gain = gain * jnp.repeat(jnp.exp(steps), dims[axis_at] // blocks).reshape((-1,) + (1,) * (len(dims) - 1 - axis_at))
    return gain


def scatter_about(stream_key, dims, deviation, bound, cuts=(), kind=jnp.bfloat16):
    result = deviation * jax.random.normal(stream_key, dims, jnp.float32)
    if cuts:
        result = result * levels(stream_key, dims, cuts, -0.22, 0.18)
    return jnp.clip(result, -bound, bound).astype(kind)


def setup_inputs(seed: int = 0) -> dict:
    streams_of = jax.random.split(jax.random.key(seed), 7)
    return {
        "traces": scatter_about(streams_of[0], (NBX, NBY, TR, NS), 1.0, 6.0, ((0, 4), (1, 8))),
        "aperture": touch_ends((jax.random.randint(streams_of[1], (NBX, NBY, 9), 0, 3) < 2).astype(jnp.int32), jax.random.fold_in(streams_of[1], 1), 0, 1),
        "geometry": draw_geometry(jax.random.fold_in(streams_of[6], 71), 0),
        "trace_weight": jnp.clip(jnp.exp(math.log(0.03515625) - 1.3862944 * jax.random.uniform(streams_of[3], (NBX, NBY, TR), jnp.float32) ** levels(streams_of[3], (NBX, NBY, TR), ((0, 4), (1, 8)), -0.2, 0.2)), 0.0087890625, 0.03515625).astype(jnp.bfloat16),
        "class_weight": jnp.clip(jnp.exp(jax.random.uniform(streams_of[4], (NC,), jnp.float32, math.log(0.3), math.log(1.5))), 0.3, 1.5),
        "traveltime": draw_traveltime(jax.random.fold_in(streams_of[6], 71), 0),
    }


def migrate(samples_in, live_weights, geometry, tile_x, tile_y, traveltime, class_weight):
    points = jnp.arange(PX * PY, dtype=jnp.int32)
    point_x = tile_x * PX + points // PY
    point_y = tile_y * PY + points % PY
    distance = jnp.abs(point_x[:, None] - geometry[0][None, :]) + jnp.abs(point_y[:, None] - geometry[1][None, :])
    classes = geometry[2][None, :] + distance // DSTEP
    sample_ids = jnp.arange(NS, dtype=jnp.int32)[:, None]
    samples_wide = samples_in.astype(jnp.float32)

    def add_class(level, image):
        scaled = (live_weights * class_weight[level]).astype(jnp.bfloat16).astype(jnp.float32)
        amplitude = jnp.where(classes == level, scaled[None, :], jnp.float32(0.0))
        stacked = jnp.dot(amplitude, samples_wide, precision=lax.Precision.HIGHEST, preferred_element_type=jnp.float32)
        quarter = traveltime[level]
        first_sample = quarter // 4
        fraction = (quarter % 4).astype(jnp.float32) * 0.25
        interp = jnp.where(sample_ids == first_sample[None, :], 1.0 - fraction[None, :], 0.0) + jnp.where(sample_ids == first_sample[None, :] + 1, fraction[None, :], 0.0)
        return image + jnp.dot(stacked, interp.astype(jnp.float32), precision=lax.Precision.HIGHEST, preferred_element_type=jnp.float32)

    return lax.fori_loop(0, class_weight.shape[0], add_class, jnp.zeros((PX * PY, NTIME), jnp.float32))


def reference(traces, aperture, geometry, trace_weight, class_weight, traveltime):
    padded_traces = jnp.pad(traces, ((BB, BB), (BB, BB), (0, 0), (0, 0)))
    padded_aperture = jnp.pad(aperture, ((BB, BB), (BB, BB), (0, 0)))
    padded_geometry = jnp.pad(geometry, ((BB, BB), (BB, BB), (0, 0), (0, 0)))
    padded_weight = jnp.pad(trace_weight, ((BB, BB), (BB, BB), (0, 0)))
    offset = jnp.arange(3 * BB, dtype=jnp.int32) // BB - 1
    wanted = (1 - offset)[:, None] * 3 + (1 - offset)[None, :]
    choose = (jnp.arange(9, dtype=jnp.int32)[None, None, :] == wanted[:, :, None]).astype(jnp.int32)
    zero_index = jnp.int32(0)

    def one_tile(tile):
        tile_x = (tile // N_GY).astype(jnp.int32)
        tile_y = (tile % N_GY).astype(jnp.int32)
        start_x = (tile_x * BB).astype(jnp.int32)
        start_y = (tile_y * BB).astype(jnp.int32)
        near_traces = lax.dynamic_slice(padded_traces, (start_x, start_y, zero_index, zero_index), (3 * BB, 3 * BB, TR, NS))
        near_aperture = lax.dynamic_slice(padded_aperture, (start_x, start_y, zero_index), (3 * BB, 3 * BB, 9))
        near_geometry = lax.dynamic_slice(padded_geometry, (start_x, start_y, zero_index, zero_index), (3 * BB, 3 * BB, 3, TR))
        near_weight = lax.dynamic_slice(padded_weight, (start_x, start_y, zero_index), (3 * BB, 3 * BB, TR))
        live_block = jnp.sum(near_aperture * choose, axis=2)
        live = jnp.broadcast_to(live_block[:, :, None], near_weight.shape).reshape(-1)
        live_weights = near_weight.reshape(-1).astype(jnp.float32) * live.astype(jnp.float32)
        flat_geometry = jnp.moveaxis(near_geometry, 2, 0).reshape(3, -1)
        return migrate(near_traces.reshape(-1, NS), live_weights, flat_geometry, tile_x, tile_y, traveltime, class_weight)

    tiles = lax.map(one_tile, jnp.arange(N_GX * N_GY, dtype=jnp.int32))
    return tiles.reshape(N_GX, N_GY, PX, PY, NTIME).transpose(0, 2, 1, 3, 4).reshape(NX, NY, NTIME)
```

```python
import functools

import jax
import jax.numpy as jnp
from jax import lax
from jax.experimental import pallas as pl
from jax.experimental.pallas import tpu as pltpu
from jax.sharding import PartitionSpec as P

PX = 16
PY = 8
DSTEP = 8
NH = 8
MESH = pl.DeviceIdType.MESH
BF = jnp.bfloat16
F32 = jnp.float32
ROWS = 16
GRID = 136.0
SHIFT = (DSTEP - 1) / (2 * DSTEP)

ND = (2 * PX - 1 + 2 * PY - 1) // DSTEP + 1
NCLASS = NH + ND - 1


def classes_at(dx, dy):
    far_x = 2 * PX - 1 if dx else PX - 1
    far_y = 2 * PY - 1 if dy else PY - 1
    return (far_x + far_y) // DSTEP + 1


def kernel(
    n_x, n_y, traces_at, geometry_at, weight_at, traveltime_at, aperture_at, class_weight_at,
    total, from_x, traces, geometry, weight, traveltime, aperture, class_weight,
    interp, digits, taps, values, amplitude, own, y_out, y_in, x_out, x_in,
    load_sem, send_sem, recv_sem,
):
    bx, by, tr, ns = traces.shape
    nt = traveltime.shape[1]
    nj = bx * by * tr
    cols = PX * PY
    blocks = [(i, k) for i in range(bx) for k in range(by)]
    pairs = [(traveltime_at, traveltime), (geometry_at, geometry), (weight_at, weight)]
    pairs += [(aperture_at, aperture), (class_weight_at, class_weight)]
    pairs += [(traces_at.at[i, k], traces.at[i, k]) for i, k in blocks]
    loads = [
        pltpu.make_async_copy(src, dst, load_sem.at[n]) for n, (src, dst) in enumerate(pairs)
    ]
    for load in loads:
        load.start()
    me_x = lax.axis_index("gx")
    me_y = lax.axis_index("gy")
    side = 2 * lax.rem(me_y, 2) - 1
    step_x = (-1, 1)
    step_y = (side, -side)
    has_x = [me_x > 0, me_x < n_x - 1]
    has_y = [jnp.logical_and(me_y + s >= 0, me_y + s < n_y) for s in step_y]
    barrier = pltpu.get_barrier_semaphore()

    def when(there, act):
        pl.when(there)(act)

    for k in range(2):
        @pl.when(has_x[k])
        def _(k=k):
            pl.semaphore_signal(
                barrier, inc=1, device_id={"gx": me_x + step_x[k]}, device_id_type=MESH
            )

        @pl.when(has_y[k])
        def _(k=k):
            pl.semaphore_signal(
                barrier, inc=1, device_id={"gy": me_y + step_y[k]}, device_id_type=MESH
            )

    def copy(src, dst, number, device):
        return pltpu.make_async_remote_copy(
            src_ref=src, dst_ref=dst,
            send_sem=send_sem.at[number], recv_sem=recv_sem.at[number],
            device_id=device, device_id_type=MESH,
        )

    along_y = [
        [copy(y_out.at[n, k], y_in.at[n, k], 2 * n + k, {"gy": me_y + step_y[k]}) for k in range(2)]
        for n in range(3)
    ]
    along_x = [
        copy(x_out.at[k], x_in.at[k], 6 + k, {"gx": me_x + step_x[k]}) for k in range(2)
    ]

    for k in range(2):
        @pl.when(jnp.logical_not(has_y[k]))
        def _(k=k):
            for n in range(3):
                y_in[n, k] = jnp.zeros(y_in.shape[2:], BF)

        @pl.when(jnp.logical_not(has_x[1 - k]))
        def _(k=k):
            x_in[k] = jnp.zeros(x_in.shape[1:], BF)

    groups = [blocks[b : b + by] for b in range(0, len(blocks), by)]
    zero = jnp.zeros((), BF)

    def spread(row):
        return jnp.broadcast_to(row, (ROWS, row.shape[1])).astype(BF)

    loads[0].wait()
    quarter = traveltime[...]
    first = (quarter >> 2).astype(F32)
    fraction = (quarter & 3).astype(F32) * 0.25
    row_ids = lax.broadcasted_iota(jnp.int32, (ROWS, nt), 0).astype(F32).astype(BF)

    def build_interp(c):
        at, part = first[c : c + 1, :], fraction[c : c + 1, :]
        at_b, next_b = spread(at), spread(at + 1.0)
        part_b, rest_b = spread(part), spread(1.0 - part)
        for r in range(0, ns, ROWS):
            ids = row_ids + BF(r)
            interp[c, pl.ds(r, ROWS), :] = jnp.where(
                ids == at_b, rest_b, jnp.where(ids == next_b, part_b, zero)
            )

    for c in range(NCLASS):
        build_interp(c)
    for load in loads[1:5]:
        load.wait()

    for b, (i, k) in enumerate(blocks):
        o = jnp.broadcast_to(geometry[i, 2, k : k + 1, :].astype(F32), (tr, tr)).T
        o = jnp.concatenate([o] * (nt // tr), axis=1).astype(BF)
        digits[pl.ds(b * tr, tr), :] = o

    def row_of(ref, r, group):
        return jnp.concatenate([ref[i, r, k : k + 1, :] for i, k in group], axis=1)

    def scaled(group, d):
        offset = row_of(geometry, 2, group)
        factor = jnp.zeros(offset.shape, F32)
        for h in range(NH):
            factor = jnp.where(offset == h, class_weight[h + d], factor)
        weights = jnp.concatenate([weight[i, k : k + 1, :] for i, k in group], axis=1).astype(F32)
        return (weights * factor).astype(BF).astype(F32)

    wide = by * tr
    scales = [[scaled(group, d) for d in range(ND)] for group in groups]
    row = lax.broadcasted_iota(jnp.int32, (ROWS, wide), 0)
    row_x = (row // PY).astype(F32).astype(BF)
    row_y = (row % PY).astype(F32).astype(BF)

    def build_amplitude(slot, dx, dy, nd, g):
        group = groups[g]
        mid_x = row_of(geometry, 0, group) - me_x * PX
        mid_y = row_of(geometry, 1, group) - me_y * PY
        at_x = row_x - spread((mid_x - dx * PX).astype(F32))
        away_y = jnp.abs(row_y - spread((mid_y - dy * PY).astype(F32)))
        away_y = away_y * BF(1 / DSTEP) - BF(SHIFT)
        entry = (dx + 1) * 3 + (dy + 1)
        live = jnp.concatenate(
            [jnp.full((1, tr), aperture[i, k, entry], jnp.int32) for i, k in group], axis=1
        ).astype(F32)
        scale = [spread(scales[g][d] * live) for d in range(nd)]
        for r in range(0, cols, ROWS):
            away_x = jnp.abs(at_x + BF(r // PY)) * BF(1 / DSTEP)
            level = (away_x + away_y) + BF(GRID)
            for d in range(nd):
                amplitude[slot, pl.ds(r, ROWS), pl.ds(d * nj + g * wide, wide)] = jnp.where(
                    level == BF(GRID + d), scale[d], zero
                )

    tiles = [(dx, dy) for dx in (-1, 1, 0) for dy in (side, -side)]
    tiles += [(dx, 0) for dx in (-1, 1, 0)]
    depths = [classes_at(dx, 1) for dx in (-1, 1, 0) for _ in range(2)]
    depths += [classes_at(dx, 0) for dx in (-1, 1, 0)]

    def amplitudes(slot):
        for g in range(len(groups)):
            build_amplitude(slot, *tiles[slot], depths[slot], g)

    def choose(r):
        rows = pl.ds(r, ROWS)
        o = digits[rows, :]
        now = [taps[c, rows, :] for c in range(NCLASS)]
        for bit in (4, 2, 1):
            take = o >= BF(bit)
            o = jnp.where(take, o - BF(bit), o)
            now = [jnp.where(take, now[c + bit], now[c]) for c in range(ND + bit - 1)]
        for d in range(ND):
            values[pl.ds(d * nj + r, ROWS), :] = now[d]

    def migrate(slot):
        total_part = None
        for g in range(len(groups)):
            left = jnp.concatenate(
                [
                    amplitude[slot, :, pl.ds(d * nj + g * wide, wide)]
                    for d in range(depths[slot])
                ],
                axis=1,
            )
            right = jnp.concatenate(
                [values[pl.ds(d * nj + g * wide, wide), :] for d in range(depths[slot])], axis=0
            )
            part = jnp.dot(left, right, preferred_element_type=F32)
            total_part = part if total_part is None else total_part + part
        return total_part

    amplitudes(0)
    for load in loads[5:]:
        load.wait()
    for g in range(len(groups)):
        for c in range(NCLASS):
            part = jnp.dot(
                traces[g].reshape(wide, ns), interp[c], preferred_element_type=F32
            )
            taps[c, pl.ds(g * wide, wide), :] = part.astype(BF)
            if g == 0 and c == 4:
                amplitudes(2)
            if g:
                count = wide // ROWS
                for r in range(c * count // NCLASS, (c + 1) * count // NCLASS):
                    choose((g - 1) * wide + r * ROWS)
    for r in range(wide // ROWS):
        choose((len(groups) - 1) * wide + r * ROWS)

    def send(n, k):
        when(has_y[k], along_y[n][k].start)

    def emit(n, k):
        y_out[n, k] = migrate(2 * n + k).astype(BF)

    emit(0, 0)
    amplitudes(1)
    there = [t.astype(jnp.int32) for t in has_x + has_y]
    pl.semaphore_wait(barrier, sum(there))
    send(0, 0)
    emit(1, 0)
    amplitudes(3)
    send(1, 0)
    emit(0, 1)
    emit(1, 1)
    amplitudes(4)
    amplitudes(5)
    send(0, 1)
    send(1, 1)
    emit(2, 0)
    emit(2, 1)
    for m in range(3):
        amplitudes(6 + m)
    send(2, 0)
    send(2, 1)
    for m in range(3):
        own[m] = migrate(6 + m)

    def summed(n):
        for k in range(2):
            when(has_y[k], along_y[n][k].wait_recv)
        return own[n] + y_in[n, 0].astype(F32) + y_in[n, 1].astype(F32)

    for k in range(2):
        x_out[k] = summed(k).astype(BF)
        when(has_x[k], along_x[k].start)
    total[...] = summed(2)
    for k in range(2):
        when(has_x[1 - k], along_x[k].wait_recv)
        from_x[k] = x_in[k]
    for k in range(2):
        for n in range(3):
            when(has_y[k], along_y[n][k].wait_send)
        when(has_x[k], along_x[k].wait_send)


def per_device(n_x, n_y, traces, aperture, geometry, trace_weight, class_weight, traveltime):
    bx, by, tr, ns = traces.shape
    nt = traveltime.shape[1]
    nj = bx * by * tr
    cols = PX * PY
    geometry = jnp.transpose(geometry, (0, 2, 1, 3))
    vmem = pl.BlockSpec(memory_space=pltpu.VMEM)
    total, from_x = pl.pallas_call(
        functools.partial(kernel, n_x, n_y),
        out_shape=(pltpu.VMEM((cols, nt), F32), pltpu.VMEM((2, cols, nt), BF)),
        in_specs=[pl.BlockSpec(memory_space=pltpu.HBM)] * 6,
        out_specs=(vmem, vmem),
        scratch_shapes=[
            pltpu.VMEM(traces.shape, traces.dtype),
            pltpu.VMEM(geometry.shape, geometry.dtype),
            pltpu.VMEM(trace_weight.shape, trace_weight.dtype),
            pltpu.VMEM(traveltime.shape, traveltime.dtype),
            pltpu.SMEM(aperture.shape, aperture.dtype),
            pltpu.SMEM(class_weight.shape, class_weight.dtype),
            pltpu.VMEM((NCLASS, ns, nt), BF),
            pltpu.VMEM((nj, nt), BF),
            pltpu.VMEM((NCLASS, nj, nt), BF),
            pltpu.VMEM((ND * nj, nt), BF),
            pltpu.VMEM((9, cols, ND * nj), BF),
            pltpu.VMEM((3, cols, nt), F32),
            pltpu.VMEM((3, 2, cols, nt), BF),
            pltpu.VMEM((3, 2, cols, nt), BF),
            pltpu.VMEM((2, cols, nt), BF),
            pltpu.VMEM((2, cols, nt), BF),
            pltpu.SemaphoreType.DMA((5 + bx * by,)),
            pltpu.SemaphoreType.DMA((8,)),
            pltpu.SemaphoreType.DMA((8,)),
        ],
        compiler_params=pltpu.CompilerParams(collective_id=0, has_side_effects=True),
    )(traces, geometry, trace_weight, traveltime, aperture, class_weight)
    image = total + from_x[0].astype(F32) + from_x[1].astype(F32)
    return image.reshape(PX, PY, nt)


def solution(mesh):
    return jax.shard_map(
        functools.partial(per_device, mesh.shape["gx"], mesh.shape["gy"]),
        mesh=mesh,
        in_specs=(
            P("gx", "gy", None, None),
            P("gx", "gy", None),
            P("gx", "gy", None, None),
            P("gx", "gy", None),
            P(),
            P(),
        ),
        out_specs=P("gx", "gy", None),
        check_vma=False,
    )
```

```python
import functools

import jax
import jax.numpy as jnp
from jax import lax
from jax.experimental import pallas as pl
from jax.experimental.pallas import tpu as pltpu
from jax.sharding import PartitionSpec as P

PX = 16
PY = 8
DSTEP = 8
NH = 8
MESH = pl.DeviceIdType.MESH
BF = jnp.bfloat16
F32 = jnp.float32
ROWS = 16
HALVES = 1
GRID = 136.0
SHIFT = (DSTEP - 1) / (2 * DSTEP)

ND = (2 * PX - 1 + 2 * PY - 1) // DSTEP + 1
NCLASS = NH + ND - 1


def classes_at(dx, dy):
    far_x = 2 * PX - 1 if dx else PX - 1
    far_y = 2 * PY - 1 if dy else PY - 1
    return (far_x + far_y) // DSTEP + 1


def kernel(
    n_x, n_y, traces_at, geometry_at, weight_at, traveltime_at, aperture_at, class_weight_at,
    total, from_x, traces, geometry, weight, traveltime, aperture, class_weight,
    interp, digits, taps, values, amplitude, own, y_out, y_in, x_out, x_in,
    load_sem, send_sem, recv_sem,
):
    bx, by, tr, ns = traces.shape
    nt = traveltime.shape[1]
    nj = bx * by * tr
    cols = PX * PY
    blocks = [(i, k) for i in range(bx) for k in range(by)]
    pairs = [(traveltime_at, traveltime), (geometry_at, geometry), (weight_at, weight)]
    pairs += [(aperture_at, aperture), (class_weight_at, class_weight)]
    pairs += [(traces_at.at[i, k], traces.at[i, k]) for i, k in blocks]
    loads = [
        pltpu.make_async_copy(src, dst, load_sem.at[n]) for n, (src, dst) in enumerate(pairs)
    ]
    for load in loads:
        load.start()
    me_x = lax.axis_index("gx")
    me_y = lax.axis_index("gy")
    side = 2 * lax.rem(me_y, 2) - 1
    step_x = (-1, 1)
    step_y = (side, -side)
    has_x = [me_x > 0, me_x < n_x - 1]
    has_y = [jnp.logical_and(me_y + s >= 0, me_y + s < n_y) for s in step_y]
    barrier = pltpu.get_barrier_semaphore()

    def when(there, act):
        pl.when(there)(act)

    for k in range(2):
        @pl.when(has_x[k])
        def _(k=k):
            pl.semaphore_signal(
                barrier, inc=1, device_id={"gx": me_x + step_x[k]}, device_id_type=MESH
            )

        @pl.when(has_y[k])
        def _(k=k):
            pl.semaphore_signal(
                barrier, inc=1, device_id={"gy": me_y + step_y[k]}, device_id_type=MESH
            )

    def copy(src, dst, number, device):
        return pltpu.make_async_remote_copy(
            src_ref=src, dst_ref=dst,
            send_sem=send_sem.at[number], recv_sem=recv_sem.at[number],
            device_id=device, device_id_type=MESH,
        )

    half = cols // HALVES

    def part_of(h):
        return pl.ds(h * half, half)

    along_y = [
        [
            [
                copy(
                    y_out.at[n, k, part_of(h)], y_in.at[n, k, part_of(h)],
                    (2 * n + k) * HALVES + h, {"gy": me_y + step_y[k]},
                )
                for h in range(HALVES)
            ]
            for k in range(2)
        ]
        for n in range(3)
    ]
    along_x = [
        [
            copy(
                x_out.at[k, part_of(h)], x_in.at[k, part_of(h)],
                (6 + k) * HALVES + h, {"gx": me_x + step_x[k]},
            )
            for h in range(HALVES)
        ]
        for k in range(2)
    ]

    for k in range(2):
        @pl.when(jnp.logical_not(has_y[k]))
        def _(k=k):
            for n in range(3):
                y_in[n, k] = jnp.zeros(y_in.shape[2:], BF)

        @pl.when(jnp.logical_not(has_x[1 - k]))
        def _(k=k):
            x_in[k] = jnp.zeros(x_in.shape[1:], BF)

    groups = [blocks[b : b + by] for b in range(0, len(blocks), by)]
    zero = jnp.zeros((), BF)

    def spread(row):
        return jnp.broadcast_to(row, (ROWS, row.shape[1])).astype(BF)

    loads[0].wait()
    quarter = traveltime[...]
    first = (quarter >> 2).astype(F32)
    fraction = (quarter & 3).astype(F32) * 0.25
    row_ids = lax.broadcasted_iota(jnp.int32, (ROWS, nt), 0).astype(F32).astype(BF)

    def build_interp(c):
        at, part = first[c : c + 1, :], fraction[c : c + 1, :]
        at_b, next_b = spread(at), spread(at + 1.0)
        part_b, rest_b = spread(part), spread(1.0 - part)
        for r in range(0, ns, ROWS):
            ids = row_ids + BF(r)
            interp[c, pl.ds(r, ROWS), :] = jnp.where(
                ids == at_b, rest_b, jnp.where(ids == next_b, part_b, zero)
            )

    for c in range(NCLASS):
        build_interp(c)
    for load in loads[1:]:
        load.wait()

    def build_digits():
        for b, (i, k) in enumerate(blocks):
            o = jnp.broadcast_to(geometry[i, 2, k : k + 1, :].astype(F32), (tr, tr)).T
            o = jnp.concatenate([o] * (nt // tr), axis=1).astype(BF)
            digits[pl.ds(b * tr, tr), :] = o

    def row_of(ref, r, group):
        return jnp.concatenate([ref[i, r, k : k + 1, :] for i, k in group], axis=1)

    def scaled(group, d):
        offset = row_of(geometry, 2, group)
        factor = jnp.zeros(offset.shape, F32)
        for h in range(NH):
            factor = jnp.where(offset == h, class_weight[h + d], factor)
        weights = jnp.concatenate([weight[i, k : k + 1, :] for i, k in group], axis=1).astype(F32)
        return (weights * factor).astype(BF).astype(F32)

    wide = by * tr
    scales = []
    row = lax.broadcasted_iota(jnp.int32, (ROWS, wide), 0)
    row_x = (row // PY).astype(F32).astype(BF)
    row_y = (row % PY).astype(F32).astype(BF)

    def amplitude_pieces(slot, g):
        (dx, dy), nd, group = tiles[slot], depths[slot], groups[g]
        mid_x = row_of(geometry, 0, group) - me_x * PX
        mid_y = row_of(geometry, 1, group) - me_y * PY
        at_x = row_x - spread((mid_x - dx * PX).astype(F32))
        away_y = jnp.abs(row_y - spread((mid_y - dy * PY).astype(F32)))
        away_y = away_y * BF(1 / DSTEP) - BF(SHIFT)
        entry = (dx + 1) * 3 + (dy + 1)
        live = jnp.concatenate(
            [jnp.full((1, tr), aperture[i, k, entry], jnp.int32) for i, k in group], axis=1
        ).astype(F32)
        scale = [spread(scales[g][d] * live) for d in range(nd)]

        def piece(r):
            away_x = jnp.abs(at_x + BF(r // PY)) * BF(1 / DSTEP)
            level = (away_x + away_y) + BF(GRID)
            for d in range(nd):
                amplitude[slot, pl.ds(r, ROWS), pl.ds(d * nj + g * wide, wide)] = jnp.where(
                    level == BF(GRID + d), scale[d], zero
                )

        return [functools.partial(piece, r) for r in range(0, cols, ROWS)]

    tiles = [(dx, dy) for dx in (-1, 1, 0) for dy in (side, -side)]
    tiles += [(dx, 0) for dx in (-1, 1, 0)]
    depths = [classes_at(dx, 1) for dx in (-1, 1, 0) for _ in range(2)]
    depths += [classes_at(dx, 0) for dx in (-1, 1, 0)]

    def amplitudes(slot):
        for g in range(len(groups)):
            for piece in amplitude_pieces(slot, g):
                piece()

    def choose(r):
        rows = pl.ds(r, ROWS)
        o = digits[rows, :]
        now = [taps[c, rows, :] for c in range(NCLASS)]
        for bit in (4, 2, 1):
            take = o >= BF(bit)
            o = jnp.where(take, o - BF(bit), o)
            now = [jnp.where(take, now[c + bit], now[c]) for c in range(ND + bit - 1)]
        for d in range(ND):
            values[pl.ds(d * nj + r, ROWS), :] = now[d]

    def migrate(slot):
        total_part = None
        for g in range(len(groups)):
            left = jnp.concatenate(
                [
                    amplitude[slot, :, pl.ds(d * nj + g * wide, wide)]
                    for d in range(depths[slot])
                ],
                axis=1,
            )
            right = jnp.concatenate(
                [values[pl.ds(d * nj + g * wide, wide), :] for d in range(depths[slot])], axis=0
            )
            part = jnp.dot(left, right, preferred_element_type=F32)
            total_part = part if total_part is None else total_part + part
        return total_part

    steps = [range(c, min(c + 2, NCLASS)) for c in range(0, NCLASS, 2)]
    for g in range(len(groups)):
        for n, classes in enumerate(steps):
            right = jnp.concatenate([interp[c] for c in classes], axis=1)
            part = jnp.dot(traces[g].reshape(wide, ns), right, preferred_element_type=F32)
            for m, c in enumerate(classes):
                taps[c, pl.ds(g * wide, wide), :] = part[:, m * nt : (m + 1) * nt].astype(BF)
            if g == 0 and n == 0:
                build_digits()
            if g == 0 and n == 1:
                scales.extend([scaled(group, d) for d in range(ND)] for group in groups)
            if g == 0 and n >= 2:
                whole = [p for q in range(len(groups)) for p in amplitude_pieces(0, q)] if n == 2 else whole
                share = len(steps) - 2
                for p in whole[(n - 2) * len(whole) // share : (n - 1) * len(whole) // share]:
                    p()
            if g:
                count = wide // ROWS
                for r in range(n * count // len(steps), (n + 1) * count // len(steps)):
                    choose((g - 1) * wide + r * ROWS)
    for r in range(wide // ROWS):
        choose((len(groups) - 1) * wide + r * ROWS)

    def send(n, k):
        for h in range(HALVES):
            when(has_y[k], along_y[n][k][h].start)

    def emit(n, k):
        y_out[n, k] = migrate(2 * n + k).astype(BF)

    emit(0, 0)
    there = [t.astype(jnp.int32) for t in has_x + has_y]
    pl.semaphore_wait(barrier, sum(there))
    send(0, 0)
    amplitudes(2)
    emit(1, 0)
    send(1, 0)
    amplitudes(1)
    amplitudes(3)
    emit(0, 1)
    emit(1, 1)
    send(0, 1)
    send(1, 1)
    amplitudes(4)
    amplitudes(5)
    emit(2, 0)
    emit(2, 1)
    send(2, 0)
    send(2, 1)
    for m in range(3):
        amplitudes(6 + m)
    for m in range(3):
        own[m] = migrate(6 + m)

    def summed(n, h):
        for k in range(2):
            when(has_y[k], along_y[n][k][h].wait_recv)
        rows = part_of(h)
        return own[n, rows] + y_in[n, 0, rows].astype(F32) + y_in[n, 1, rows].astype(F32)

    for k in range(2):
        for h in range(HALVES):
            x_out[k, part_of(h)] = summed(k, h).astype(BF)
            when(has_x[k], along_x[k][h].start)
    for h in range(HALVES):
        total[part_of(h), :] = summed(2, h)
    for k in range(2):
        for h in range(HALVES):
            when(has_x[1 - k], along_x[k][h].wait_recv)
            from_x[k, part_of(h)] = x_in[k, part_of(h)]
    for k in range(2):
        for h in range(HALVES):
            for n in range(3):
                when(has_y[k], along_y[n][k][h].wait_send)
            when(has_x[k], along_x[k][h].wait_send)


def per_device(n_x, n_y, traces, aperture, geometry, trace_weight, class_weight, traveltime):
    bx, by, tr, ns = traces.shape
    nt = traveltime.shape[1]
    nj = bx * by * tr
    cols = PX * PY
    geometry = jnp.transpose(geometry, (0, 2, 1, 3))
    vmem = pl.BlockSpec(memory_space=pltpu.VMEM)
    total, from_x = pl.pallas_call(
        functools.partial(kernel, n_x, n_y),
        out_shape=(pltpu.VMEM((cols, nt), F32), pltpu.VMEM((2, cols, nt), BF)),
        in_specs=[pl.BlockSpec(memory_space=pltpu.HBM)] * 6,
        out_specs=(vmem, vmem),
        scratch_shapes=[
            pltpu.VMEM(traces.shape, traces.dtype),
            pltpu.VMEM(geometry.shape, geometry.dtype),
            pltpu.VMEM(trace_weight.shape, trace_weight.dtype),
            pltpu.VMEM(traveltime.shape, traveltime.dtype),
            pltpu.SMEM(aperture.shape, aperture.dtype),
            pltpu.SMEM(class_weight.shape, class_weight.dtype),
            pltpu.VMEM((NCLASS, ns, nt), BF),
            pltpu.VMEM((nj, nt), BF),
            pltpu.VMEM((NCLASS, nj, nt), BF),
            pltpu.VMEM((ND * nj, nt), BF),
            pltpu.VMEM((9, cols, ND * nj), BF),
            pltpu.VMEM((3, cols, nt), F32),
            pltpu.VMEM((3, 2, cols, nt), BF),
            pltpu.VMEM((3, 2, cols, nt), BF),
            pltpu.VMEM((2, cols, nt), BF),
            pltpu.VMEM((2, cols, nt), BF),
            pltpu.SemaphoreType.DMA((5 + bx * by,)),
            pltpu.SemaphoreType.DMA((8 * HALVES,)),
            pltpu.SemaphoreType.DMA((8 * HALVES,)),
        ],
        compiler_params=pltpu.CompilerParams(collective_id=0, has_side_effects=True),
    )(traces, geometry, trace_weight, traveltime, aperture, class_weight)
    image = total + from_x[0].astype(F32) + from_x[1].astype(F32)
    return image.reshape(PX, PY, nt)


def solution(mesh):
    return jax.shard_map(
        functools.partial(per_device, mesh.shape["gx"], mesh.shape["gy"]),
        mesh=mesh,
        in_specs=(
            P("gx", "gy", None, None),
            P("gx", "gy", None),
            P("gx", "gy", None, None),
            P("gx", "gy", None),
            P(),
            P(),
        ),
        out_specs=P("gx", "gy", None),
        check_vma=False,
    )
```

```python
import functools

import jax
import jax.numpy as jnp
from jax import lax
from jax.experimental import pallas as pl
from jax.experimental.pallas import tpu as pltpu
from jax.sharding import PartitionSpec as P

PX = 16
PY = 8
DSTEP = 8
NH = 8
MESH = pl.DeviceIdType.MESH
BF = jnp.bfloat16
F32 = jnp.float32
ROWS = 16
HALVES = 1
GRID = 136.0
SHIFT = (DSTEP - 1) / (2 * DSTEP)

ND = (2 * PX - 1 + 2 * PY - 1) // DSTEP + 1
NCLASS = NH + ND - 1


def classes_at(dx, dy):
    far_x = 2 * PX - 1 if dx else PX - 1
    far_y = 2 * PY - 1 if dy else PY - 1
    return (far_x + far_y) // DSTEP + 1


def kernel(
    n_x, n_y, traces_at, geometry_at, weight_at, traveltime_at, aperture_at, class_weight_at,
    total, from_x, traces, geometry, weight, traveltime, aperture, class_weight,
    interp, digits, taps, values, amplitude, own, y_out, y_in, x_out,
    load_sem, send_sem, recv_sem,
):
    bx, by, tr, ns = traces.shape
    nt = traveltime.shape[1]
    nj = bx * by * tr
    cols = PX * PY
    blocks = [(i, k) for i in range(bx) for k in range(by)]
    pairs = [(traveltime_at, traveltime), (geometry_at, geometry), (weight_at, weight)]
    pairs += [(aperture_at, aperture), (class_weight_at, class_weight)]
    pairs += [(traces_at.at[i, k], traces.at[i, k]) for i, k in blocks]
    loads = [
        pltpu.make_async_copy(src, dst, load_sem.at[n]) for n, (src, dst) in enumerate(pairs)
    ]
    for load in loads:
        load.start()
    me_x = lax.axis_index("gx")
    me_y = lax.axis_index("gy")
    side = 2 * lax.rem(me_y, 2) - 1
    step_x = (-1, 1)
    step_y = (side, -side)
    has_x = [me_x > 0, me_x < n_x - 1]
    has_y = [jnp.logical_and(me_y + s >= 0, me_y + s < n_y) for s in step_y]
    barrier = pltpu.get_barrier_semaphore()

    def when(there, act):
        pl.when(there)(act)

    for k in range(2):
        @pl.when(has_x[k])
        def _(k=k):
            pl.semaphore_signal(
                barrier, inc=1, device_id={"gx": me_x + step_x[k]}, device_id_type=MESH
            )

        @pl.when(has_y[k])
        def _(k=k):
            pl.semaphore_signal(
                barrier, inc=1, device_id={"gy": me_y + step_y[k]}, device_id_type=MESH
            )

    def copy(src, dst, number, device):
        return pltpu.make_async_remote_copy(
            src_ref=src, dst_ref=dst,
            send_sem=send_sem.at[number], recv_sem=recv_sem.at[number],
            device_id=device, device_id_type=MESH,
        )

    half = cols // HALVES

    def part_of(h):
        return pl.ds(h * half, half)

    along_y = [
        [
            [
                copy(
                    y_out.at[n, k, part_of(h)], y_in.at[n, k, part_of(h)],
                    (2 * n + k) * HALVES + h, {"gy": me_y + step_y[k]},
                )
                for h in range(HALVES)
            ]
            for k in range(2)
        ]
        for n in range(3)
    ]
    along_x = [
        [
            copy(
                x_out.at[k, part_of(h)], from_x.at[k, part_of(h)],
                (6 + k) * HALVES + h, {"gx": me_x + step_x[k]},
            )
            for h in range(HALVES)
        ]
        for k in range(2)
    ]

    for k in range(2):
        @pl.when(jnp.logical_not(has_y[k]))
        def _(k=k):
            for n in range(3):
                y_in[n, k] = jnp.zeros(y_in.shape[2:], BF)

        @pl.when(jnp.logical_not(has_x[1 - k]))
        def _(k=k):
            from_x[k] = jnp.zeros(from_x.shape[1:], BF)

    groups = [blocks[b : b + by] for b in range(0, len(blocks), by)]
    zero = jnp.zeros((), BF)

    def spread(row):
        return jnp.broadcast_to(row, (ROWS, row.shape[1])).astype(BF)

    loads[0].wait()
    quarter = traveltime[...]
    first = (quarter >> 2).astype(F32)
    fraction = (quarter & 3).astype(F32) * 0.25
    row_ids = lax.broadcasted_iota(jnp.int32, (ROWS, nt), 0).astype(F32).astype(BF)

    def build_interp(c):
        at, part = first[c : c + 1, :], fraction[c : c + 1, :]
        at_b, next_b = spread(at), spread(at + 1.0)
        part_b, rest_b = spread(part), spread(1.0 - part)
        for r in range(0, ns, ROWS):
            ids = row_ids + BF(r)
            interp[c, pl.ds(r, ROWS), :] = jnp.where(
                ids == at_b, rest_b, jnp.where(ids == next_b, part_b, zero)
            )

    for c in range(NCLASS):
        build_interp(c)
    for load in loads[1:]:
        load.wait()

    def build_digits():
        for b, (i, k) in enumerate(blocks):
            o = jnp.broadcast_to(geometry[i, 2, k : k + 1, :].astype(F32), (tr, tr)).T
            o = jnp.concatenate([o] * (nt // tr), axis=1).astype(BF)
            digits[pl.ds(b * tr, tr), :] = o

    def row_of(ref, r, group):
        return jnp.concatenate([ref[i, r, k : k + 1, :] for i, k in group], axis=1)

    def scaled(group, d):
        offset = row_of(geometry, 2, group)
        factor = jnp.zeros(offset.shape, F32)
        for h in range(NH):
            factor = jnp.where(offset == h, class_weight[h + d], factor)
        weights = jnp.concatenate([weight[i, k : k + 1, :] for i, k in group], axis=1).astype(F32)
        return (weights * factor).astype(BF).astype(F32)

    wide = by * tr
    scales = []
    row = lax.broadcasted_iota(jnp.int32, (ROWS, wide), 0)
    row_x = (row // PY).astype(F32).astype(BF)
    row_y = (row % PY).astype(F32).astype(BF)

    def amplitude_pieces(slot, g):
        (dx, dy), nd, group = tiles[slot], depths[slot], groups[g]
        mid_x = row_of(geometry, 0, group) - me_x * PX
        mid_y = row_of(geometry, 1, group) - me_y * PY
        at_x = row_x - spread((mid_x - dx * PX).astype(F32))
        away_y = jnp.abs(row_y - spread((mid_y - dy * PY).astype(F32)))
        away_y = away_y * BF(1 / DSTEP) - BF(SHIFT)
        entry = (dx + 1) * 3 + (dy + 1)
        live = jnp.concatenate(
            [jnp.full((1, tr), aperture[i, k, entry], jnp.int32) for i, k in group], axis=1
        ).astype(F32)
        scale = [spread(scales[g][d] * live) for d in range(nd)]

        def piece(r):
            away_x = jnp.abs(at_x + BF(r // PY)) * BF(1 / DSTEP)
            level = (away_x + away_y) + BF(GRID)
            for d in range(nd):
                amplitude[slot, pl.ds(r, ROWS), pl.ds(d * nj + g * wide, wide)] = jnp.where(
                    level == BF(GRID + d), scale[d], zero
                )

        return [functools.partial(piece, r) for r in range(0, cols, ROWS)]

    tiles = [(dx, dy) for dx in (-1, 1, 0) for dy in (side, -side)]
    tiles += [(dx, 0) for dx in (-1, 1, 0)]
    depths = [classes_at(dx, 1) for dx in (-1, 1, 0) for _ in range(2)]
    depths += [classes_at(dx, 0) for dx in (-1, 1, 0)]

    def amplitudes(slot):
        for g in range(len(groups)):
            for piece in amplitude_pieces(slot, g):
                piece()

    def keep(c, now):
        taps[c] = now

    def choose(r):
        rows = pl.ds(r, ROWS)
        o = digits[rows, :]
        now = [taps[c, rows, :] for c in range(NCLASS)]
        for bit in (4, 2, 1):
            take = o >= BF(bit)
            o = jnp.where(take, o - BF(bit), o)
            now = [jnp.where(take, now[c + bit], now[c]) for c in range(ND + bit - 1)]
        for d in range(ND):
            values[pl.ds(d * nj + r, ROWS), :] = now[d]

    def migrate(slot):
        total_part = None
        for g in range(len(groups)):
            left = jnp.concatenate(
                [
                    amplitude[slot, :, pl.ds(d * nj + g * wide, wide)]
                    for d in range(depths[slot])
                ],
                axis=1,
            )
            right = jnp.concatenate(
                [values[pl.ds(d * nj + g * wide, wide), :] for d in range(depths[slot])], axis=0
            )
            part = jnp.dot(left, right, preferred_element_type=F32)
            total_part = part if total_part is None else total_part + part
        return total_part

    steps = [range(c, min(c + 2, NCLASS)) for c in range(0, NCLASS, 2)]
    for n, classes in enumerate(steps):
        right = jnp.concatenate([interp[c] for c in classes], axis=1)
        part = jnp.dot(traces[...].reshape(nj, ns), right, preferred_element_type=F32)
        for m, c in enumerate(classes):
            now = part[:, m * nt : (m + 1) * nt].astype(BF)
            keep(c, now)
        if n == 0:
            build_digits()
        if n == 1:
            scales.extend([scaled(group, d) for d in range(ND)] for group in groups)
        if n == 2:
            whole = [p for q in range(len(groups)) for p in amplitude_pieces(0, q)]
        if n >= 2:
            share = len(steps) - 2
            for p in whole[(n - 2) * len(whole) // share : (n - 1) * len(whole) // share]:
                p()
    for r in range(0, nj, ROWS):
        choose(r)

    def send(n, k):
        for h in range(HALVES):
            when(has_y[k], along_y[n][k][h].start)

    def emit(n, k):
        y_out[n, k] = migrate(2 * n + k).astype(BF)

    emit(0, 0)
    there = [t.astype(jnp.int32) for t in has_x + has_y]
    pl.semaphore_wait(barrier, sum(there))
    send(0, 0)
    amplitudes(2)
    emit(1, 0)
    send(1, 0)
    amplitudes(1)
    amplitudes(3)
    emit(0, 1)
    emit(1, 1)
    send(0, 1)
    send(1, 1)
    amplitudes(4)
    amplitudes(5)
    emit(2, 0)
    emit(2, 1)
    send(2, 0)
    send(2, 1)
    for m in range(3):
        amplitudes(6 + m)
    for m in range(3):
        own[m] = migrate(6 + m)

    def summed(n, h):
        for k in range(2):
            when(has_y[k], along_y[n][k][h].wait_recv)
        rows = part_of(h)
        return own[n, rows] + y_in[n, 0, rows].astype(F32) + y_in[n, 1, rows].astype(F32)

    for k in range(2):
        for h in range(HALVES):
            x_out[k, part_of(h)] = summed(k, h).astype(BF)
            when(has_x[k], along_x[k][h].start)
    for h in range(HALVES):
        total[part_of(h), :] = summed(2, h)
    for k in range(2):
        for h in range(HALVES):
            when(has_x[1 - k], along_x[k][h].wait_recv)
    for k in range(2):
        for h in range(HALVES):
            for n in range(3):
                when(has_y[k], along_y[n][k][h].wait_send)
            when(has_x[k], along_x[k][h].wait_send)


def per_device(n_x, n_y, traces, aperture, geometry, trace_weight, class_weight, traveltime):
    bx, by, tr, ns = traces.shape
    nt = traveltime.shape[1]
    nj = bx * by * tr
    cols = PX * PY
    geometry = jnp.transpose(geometry, (0, 2, 1, 3))
    vmem = pl.BlockSpec(memory_space=pltpu.VMEM)
    total, from_x = pl.pallas_call(
        functools.partial(kernel, n_x, n_y),
        out_shape=(pltpu.VMEM((cols, nt), F32), pltpu.VMEM((2, cols, nt), BF)),
        in_specs=[pl.BlockSpec(memory_space=pltpu.HBM)] * 6,
        out_specs=(vmem, vmem),
        scratch_shapes=[
            pltpu.VMEM(traces.shape, traces.dtype),
            pltpu.VMEM(geometry.shape, geometry.dtype),
            pltpu.VMEM(trace_weight.shape, trace_weight.dtype),
            pltpu.VMEM(traveltime.shape, traveltime.dtype),
            pltpu.SMEM(aperture.shape, aperture.dtype),
            pltpu.SMEM(class_weight.shape, class_weight.dtype),
            pltpu.VMEM((NCLASS, ns, nt), BF),
            pltpu.VMEM((nj, nt), BF),
            pltpu.VMEM((NCLASS, nj, nt), BF),
            pltpu.VMEM((ND * nj, nt), BF),
            pltpu.VMEM((9, cols, ND * nj), BF),
            pltpu.VMEM((3, cols, nt), F32),
            pltpu.VMEM((3, 2, cols, nt), BF),
            pltpu.VMEM((3, 2, cols, nt), BF),
            pltpu.VMEM((2, cols, nt), BF),
            pltpu.SemaphoreType.DMA((5 + bx * by,)),
            pltpu.SemaphoreType.DMA((8 * HALVES,)),
            pltpu.SemaphoreType.DMA((8 * HALVES,)),
        ],
        compiler_params=pltpu.CompilerParams(collective_id=0, has_side_effects=True),
    )(traces, geometry, trace_weight, traveltime, aperture, class_weight)
    image = total + from_x[0].astype(F32) + from_x[1].astype(F32)
    return image.reshape(PX, PY, nt)


def solution(mesh):
    return jax.shard_map(
        functools.partial(per_device, mesh.shape["gx"], mesh.shape["gy"]),
        mesh=mesh,
        in_specs=(
            P("gx", "gy", None, None),
            P("gx", "gy", None),
            P("gx", "gy", None, None),
            P("gx", "gy", None),
            P(),
            P(),
        ),
        out_specs=P("gx", "gy", None),
        check_vma=False,
    )
```

```python
import functools

import jax
import jax.numpy as jnp
from jax import lax
from jax.experimental import pallas as pl
from jax.experimental.pallas import tpu as pltpu
from jax.sharding import PartitionSpec as P

PX = 16
PY = 8
DSTEP = 8
NH = 8
MESH = pl.DeviceIdType.MESH
BF = jnp.bfloat16
F32 = jnp.float32
ROWS = 16
HALVES = 1
GRID = 136.0
SHIFT = (DSTEP - 1) / (2 * DSTEP)

ND = (2 * PX - 1 + 2 * PY - 1) // DSTEP + 1
NCLASS = NH + ND - 1


def classes_at(dx, dy):
    far_x = 2 * PX - 1 if dx else PX - 1
    far_y = 2 * PY - 1 if dy else PY - 1
    return (far_x + far_y) // DSTEP + 1


def kernel(
    n_x, n_y, traces_at, geometry_at, weight_at, traveltime_at, aperture_at, class_weight_at,
    total, from_x, traces, geometry, weight, traveltime, aperture, class_weight,
    interp, digits, taps, values, amplitude, own, y_out, y_in, x_out,
    load_sem, send_sem, recv_sem,
):
    bx, by, tr, ns = traces.shape
    nt = traveltime.shape[1]
    nj = bx * by * tr
    cols = PX * PY
    blocks = [(i, k) for i in range(bx) for k in range(by)]
    pairs = [(traveltime_at, traveltime), (geometry_at, geometry), (weight_at, weight)]
    pairs += [(aperture_at, aperture), (class_weight_at, class_weight)]
    pairs += [(traces_at.at[i, k], traces.at[i, k]) for i, k in blocks]
    loads = [
        pltpu.make_async_copy(src, dst, load_sem.at[n]) for n, (src, dst) in enumerate(pairs)
    ]
    for load in loads:
        load.start()
    me_x = lax.axis_index("gx")
    me_y = lax.axis_index("gy")
    side = 2 * lax.rem(me_y, 2) - 1
    step_x = (-1, 1)
    step_y = (side, -side)
    has_x = [me_x > 0, me_x < n_x - 1]
    has_y = [jnp.logical_and(me_y + s >= 0, me_y + s < n_y) for s in step_y]
    barrier = pltpu.get_barrier_semaphore()

    def when(there, act):
        pl.when(there)(act)

    for k in range(2):
        @pl.when(has_x[k])
        def _(k=k):
            pl.semaphore_signal(
                barrier, inc=1, device_id={"gx": me_x + step_x[k]}, device_id_type=MESH
            )

        @pl.when(has_y[k])
        def _(k=k):
            pl.semaphore_signal(
                barrier, inc=1, device_id={"gy": me_y + step_y[k]}, device_id_type=MESH
            )

    def copy(src, dst, number, device):
        return pltpu.make_async_remote_copy(
            src_ref=src, dst_ref=dst,
            send_sem=send_sem.at[number], recv_sem=recv_sem.at[number],
            device_id=device, device_id_type=MESH,
        )

    half = cols // HALVES

    def part_of(h):
        return pl.ds(h * half, half)

    along_y = [
        [
            [
                copy(
                    y_out.at[n, k, part_of(h)], y_in.at[n, k, part_of(h)],
                    (2 * n + k) * HALVES + h, {"gy": me_y + step_y[k]},
                )
                for h in range(HALVES)
            ]
            for k in range(2)
        ]
        for n in range(3)
    ]
    along_x = [
        [
            copy(
                x_out.at[k, part_of(h)], from_x.at[k, part_of(h)],
                (6 + k) * HALVES + h, {"gx": me_x + step_x[k]},
            )
            for h in range(HALVES)
        ]
        for k in range(2)
    ]

    for k in range(2):
        @pl.when(jnp.logical_not(has_y[k]))
        def _(k=k):
            for n in range(3):
                y_in[n, k] = jnp.zeros(y_in.shape[2:], BF)

        @pl.when(jnp.logical_not(has_x[1 - k]))
        def _(k=k):
            from_x[k] = jnp.zeros(from_x.shape[1:], BF)

    groups = [blocks[b : b + by] for b in range(0, len(blocks), by)]
    zero = jnp.zeros((), BF)

    def spread(row):
        return jnp.broadcast_to(row, (ROWS, row.shape[1])).astype(BF)

    loads[0].wait()
    quarter = traveltime[...]
    first = (quarter >> 2).astype(F32)
    fraction = (quarter & 3).astype(F32) * 0.25
    row_ids = lax.broadcasted_iota(jnp.int32, (ROWS, nt), 0).astype(F32).astype(BF)

    def build_interp(c):
        at, part = first[c : c + 1, :], fraction[c : c + 1, :]
        at_b, next_b = spread(at), spread(at + 1.0)
        part_b, rest_b = spread(part), spread(1.0 - part)
        for r in range(0, ns, ROWS):
            ids = row_ids + BF(r)
            interp[c, pl.ds(r, ROWS), :] = jnp.where(
                ids == at_b, rest_b, jnp.where(ids == next_b, part_b, zero)
            )

    for c in range(NCLASS):
        build_interp(c)
    for load in loads[1:]:
        load.wait()

    def build_digits():
        for b, (i, k) in enumerate(blocks):
            o = jnp.broadcast_to(geometry[i, 2, k : k + 1, :].astype(F32), (tr, tr)).T
            o = jnp.concatenate([o] * (nt // tr), axis=1).astype(BF)
            digits[pl.ds(b * tr, tr), :] = o

    def row_of(ref, r, group):
        return jnp.concatenate([ref[i, r, k : k + 1, :] for i, k in group], axis=1)

    def scaled(group, d):
        offset = row_of(geometry, 2, group)
        factor = jnp.zeros(offset.shape, F32)
        for h in range(NH):
            factor = jnp.where(offset == h, class_weight[h + d], factor)
        weights = jnp.concatenate([weight[i, k : k + 1, :] for i, k in group], axis=1).astype(F32)
        return (weights * factor).astype(BF).astype(F32)

    wide = by * tr
    scales = []
    row = lax.broadcasted_iota(jnp.int32, (ROWS, wide), 0)
    row_x = (row // PY).astype(F32).astype(BF)
    row_y = (row % PY).astype(F32).astype(BF)

    def amplitude_pieces(slot, g):
        (dx, dy), nd, group = tiles[slot], depths[slot], groups[g]
        mid_x = row_of(geometry, 0, group) - me_x * PX
        mid_y = row_of(geometry, 1, group) - me_y * PY
        at_x = row_x - spread((mid_x - dx * PX).astype(F32))
        away_y = jnp.abs(row_y - spread((mid_y - dy * PY).astype(F32)))
        away_y = away_y * BF(1 / DSTEP) - BF(SHIFT)
        entry = (dx + 1) * 3 + (dy + 1)
        live = jnp.concatenate(
            [jnp.full((1, tr), aperture[i, k, entry], jnp.int32) for i, k in group], axis=1
        ).astype(F32)
        scale = [spread(scales[g][d] * live) for d in range(nd)]

        def piece(r):
            away_x = jnp.abs(at_x + BF(r // PY)) * BF(1 / DSTEP)
            level = (away_x + away_y) + BF(GRID)
            for d in range(nd):
                amplitude[slot, pl.ds(r, ROWS), pl.ds(d * nj + g * wide, wide)] = jnp.where(
                    level == BF(GRID + d), scale[d], zero
                )

        return [functools.partial(piece, r) for r in range(0, cols, ROWS)]

    tiles = [(dx, dy) for dx in (-1, 1, 0) for dy in (side, -side)]
    tiles += [(dx, 0) for dx in (-1, 1, 0)]
    depths = [classes_at(dx, 1) for dx in (-1, 1, 0) for _ in range(2)]
    depths += [classes_at(dx, 0) for dx in (-1, 1, 0)]

    def amplitudes(slot):
        for g in range(len(groups)):
            for piece in amplitude_pieces(slot, g):
                piece()

    def keep(c, now):
        taps[c] = now

    def choose(r):
        rows = pl.ds(r, ROWS)
        o = digits[rows, :]
        now = [taps[c, rows, :] for c in range(NCLASS)]
        for bit in (4, 2, 1):
            take = o >= BF(bit)
            o = jnp.where(take, o - BF(bit), o)
            now = [jnp.where(take, now[c + bit], now[c]) for c in range(ND + bit - 1)]
        for d in range(ND):
            values[pl.ds(d * nj + r, ROWS), :] = now[d]

    def migrate(slot):
        total_part = None
        for g in range(len(groups)):
            left = jnp.concatenate(
                [
                    amplitude[slot, :, pl.ds(d * nj + g * wide, wide)]
                    for d in range(depths[slot])
                ],
                axis=1,
            )
            right = jnp.concatenate(
                [values[pl.ds(d * nj + g * wide, wide), :] for d in range(depths[slot])], axis=0
            )
            part = jnp.dot(left, right, preferred_element_type=F32)
            total_part = part if total_part is None else total_part + part
        return total_part

    steps = [range(c, min(c + 2, NCLASS)) for c in range(0, NCLASS, 2)]
    for n, classes in enumerate(steps):
        right = jnp.concatenate([interp[c] for c in classes], axis=1)
        part = jnp.dot(traces[...].reshape(nj, ns), right, preferred_element_type=F32)
        for m, c in enumerate(classes):
            now = part[:, m * nt : (m + 1) * nt].astype(BF)
            keep(c, now)
        if n == 0:
            build_digits()
        if n == 1:
            scales.extend([scaled(group, d) for d in range(ND)] for group in groups)
        if n == 2:
            whole = [p for q in range(len(groups)) for p in amplitude_pieces(0, q)]
        if n >= 2:
            share = len(steps) - 2
            for p in whole[(n - 2) * len(whole) // share : (n - 1) * len(whole) // share]:
                p()
    for r in range(0, nj, ROWS):
        choose(r)

    def send(n, k):
        for h in range(HALVES):
            when(has_y[k], along_y[n][k][h].start)

    def emit(n, k):
        y_out[n, k] = migrate(2 * n + k).astype(BF)

    emit(0, 0)
    there = [t.astype(jnp.int32) for t in has_x + has_y]
    pl.semaphore_wait(barrier, sum(there))
    send(0, 0)
    amplitudes(2)
    emit(1, 0)
    send(1, 0)
    amplitudes(1)
    amplitudes(3)
    emit(0, 1)
    emit(1, 1)
    send(0, 1)
    send(1, 1)
    for m in range(2):
        amplitudes(6 + m)
    for m in range(2):
        own[m] = migrate(6 + m)
    amplitudes(4)
    amplitudes(5)
    emit(2, 0)
    emit(2, 1)
    send(2, 0)
    send(2, 1)

    def summed(n, h):
        for k in range(2):
            when(has_y[k], along_y[n][k][h].wait_recv)
        rows = part_of(h)
        return own[n, rows] + y_in[n, 0, rows].astype(F32) + y_in[n, 1, rows].astype(F32)

    for k in range(2):
        for h in range(HALVES):
            x_out[k, part_of(h)] = summed(k, h).astype(BF)
            when(has_x[k], along_x[k][h].start)
    amplitudes(8)
    own[2] = migrate(8)
    for h in range(HALVES):
        total[part_of(h), :] = summed(2, h)
    for k in range(2):
        for h in range(HALVES):
            when(has_x[1 - k], along_x[k][h].wait_recv)
    for k in range(2):
        for h in range(HALVES):
            for n in range(3):
                when(has_y[k], along_y[n][k][h].wait_send)
            when(has_x[k], along_x[k][h].wait_send)


def per_device(n_x, n_y, traces, aperture, geometry, trace_weight, class_weight, traveltime):
    bx, by, tr, ns = traces.shape
    nt = traveltime.shape[1]
    nj = bx * by * tr
    cols = PX * PY
    geometry = jnp.transpose(geometry, (0, 2, 1, 3))
    vmem = pl.BlockSpec(memory_space=pltpu.VMEM)
    total, from_x = pl.pallas_call(
        functools.partial(kernel, n_x, n_y),
        out_shape=(pltpu.VMEM((cols, nt), F32), pltpu.VMEM((2, cols, nt), BF)),
        in_specs=[pl.BlockSpec(memory_space=pltpu.HBM)] * 6,
        out_specs=(vmem, vmem),
        scratch_shapes=[
            pltpu.VMEM(traces.shape, traces.dtype),
            pltpu.VMEM(geometry.shape, geometry.dtype),
            pltpu.VMEM(trace_weight.shape, trace_weight.dtype),
            pltpu.VMEM(traveltime.shape, traveltime.dtype),
            pltpu.SMEM(aperture.shape, aperture.dtype),
            pltpu.SMEM(class_weight.shape, class_weight.dtype),
            pltpu.VMEM((NCLASS, ns, nt), BF),
            pltpu.VMEM((nj, nt), BF),
            pltpu.VMEM((NCLASS, nj, nt), BF),
            pltpu.VMEM((ND * nj, nt), BF),
            pltpu.VMEM((9, cols, ND * nj), BF),
            pltpu.VMEM((3, cols, nt), F32),
            pltpu.VMEM((3, 2, cols, nt), BF),
            pltpu.VMEM((3, 2, cols, nt), BF),
            pltpu.VMEM((2, cols, nt), BF),
            pltpu.SemaphoreType.DMA((5 + bx * by,)),
            pltpu.SemaphoreType.DMA((8 * HALVES,)),
            pltpu.SemaphoreType.DMA((8 * HALVES,)),
        ],
        compiler_params=pltpu.CompilerParams(collective_id=0, has_side_effects=True),
    )(traces, geometry, trace_weight, traveltime, aperture, class_weight)
    image = total + from_x[0].astype(F32) + from_x[1].astype(F32)
    return image.reshape(PX, PY, nt)


def solution(mesh):
    return jax.shard_map(
        functools.partial(per_device, mesh.shape["gx"], mesh.shape["gy"]),
        mesh=mesh,
        in_specs=(
            P("gx", "gy", None, None),
            P("gx", "gy", None),
            P("gx", "gy", None, None),
            P("gx", "gy", None),
            P(),
            P(),
        ),
        out_specs=P("gx", "gy", None),
        check_vma=False,
    )
```
